32 devices in a mesh: batch: 1 (over z), ysp: 4 (over y), xsp: 8 (over x, core).
Axes of the slice: x: 4, y: 4, z: 1, core: 2. Of those that a mesh axis runs over, the one named last changes fastest.
The devices are a block of a 4x4x8 slice.
Arguments:
- volume: bfloat16 [64, 256, 128, 128], P('batch', 'xsp', 'ysp')
- filter_taps: float32 [3, 3, 21], replicated
- mix_weights: bfloat16 [3, 64, 64], replicated
- mix_bias: float32 [3, 64], replicated
Outputs:
- output: bfloat16 [64, 256, 128, 128], P('batch', 'xsp', 'ysp')
All inputs are finite; a program needn't handle non-finite values.
Results may differ from the reference program's by a relative error of at most 0.00648.
Values are sent between devices in bfloat16 or wider.
A program may use at most 768 MiB of HBM per device.

```python
import jax
import jax.numpy as jnp
from jax import lax

CHANNELS = 64
FILTER_TAPS = 21
LAYERS = 3
GRID_X = 256
GRID_Y = 128
GRID_Z = 128
HALF_WIDTH = (FILTER_TAPS - 1) // 2


def setup_inputs(seed: int = 0, part: int = 0) -> dict:
    vol_key = jax.random.fold_in(jax.random.key(seed), part)
    key_sign, key_mag, key_mix, key_bias = jax.random.split(jax.random.key(seed + 1), 4)
    volume = jax.random.normal(vol_key, (CHANNELS, GRID_X, GRID_Y, GRID_Z), jnp.float32)
    tap_signs = jnp.where(jax.random.bernoulli(key_sign, 0.5, (LAYERS, 3, FILTER_TAPS)), 1.0, -1.0)
    tap_mags = jax.random.uniform(key_mag, (LAYERS, 3, FILTER_TAPS), jnp.float32, 0.5, 1.0)
    raw_taps = tap_signs * tap_mags
    filter_taps = raw_taps / jnp.sqrt(jnp.sum(raw_taps * raw_taps, axis=-1, keepdims=True))
    mix_weights = jax.random.normal(key_mix, (LAYERS, CHANNELS, CHANNELS), jnp.float32) * CHANNELS ** -0.5
    mix_bias = 0.5 * jax.random.normal(key_bias, (LAYERS, CHANNELS), jnp.float32)
    return {"volume": volume.astype(jnp.bfloat16), "filter_taps": filter_taps, "mix_weights": mix_weights.astype(jnp.bfloat16), "mix_bias": mix_bias}


def line_filter(channel_vol, tap_row, dim_index):
    extent = channel_vol.shape[dim_index]
    pad_cfg = [(0, 0), (0, 0), (0, 0)]
    pad_cfg[dim_index] = (HALF_WIDTH, HALF_WIDTH)
    padded = jnp.pad(channel_vol.astype(jnp.float32), pad_cfg)
    tap_vals = tap_row.astype(jnp.bfloat16).astype(jnp.float32)
    accum_sum = jnp.zeros(channel_vol.shape, jnp.float32)
    for tap_pos in range(FILTER_TAPS):
        accum_sum = accum_sum + tap_vals[tap_pos] * lax.slice_in_dim(padded, tap_pos, tap_pos + extent, axis=dim_index)
    return accum_sum.astype(jnp.bfloat16)


def reference(volume, filter_taps, mix_weights, mix_bias):
    def layer_step(current, params):
        tap_set, mix_mat, bias_vec = params

        def filter_channel(channel_vol):
            x_filtered = line_filter(channel_vol, tap_set[0], 0)
            xy_filtered = line_filter(x_filtered, tap_set[1], 1)
            return line_filter(xy_filtered, tap_set[2], 2)

        smooth = lax.map(filter_channel, current)
        mix_f32 = mix_mat.astype(jnp.float32)

        def mix_plane(pair):
            plane_u, plane_v = pair
            pre_act = jnp.einsum("cd,cyz->dyz", mix_f32, plane_u.astype(jnp.float32)) + bias_vec[:, None, None]
            return (plane_v.astype(jnp.float32) + jax.nn.gelu(pre_act, approximate=True)).astype(jnp.bfloat16)

        planes = lax.map(mix_plane, (jnp.moveaxis(smooth, 1, 0), jnp.moveaxis(current, 1, 0)))
        return jnp.moveaxis(planes, 0, 1), None

    result, _ = lax.scan(layer_step, volume, (filter_taps, mix_weights, mix_bias))
    return result
```

```python
import functools

import jax
import jax.numpy as jnp
from jax import lax
from jax.experimental import pallas as pl
from jax.experimental.pallas import tpu as pltpu
from jax.sharding import PartitionSpec as P

PARTS_AXIS = "batch"
COL_AXIS = "ysp"
ROW_AXIS = "xsp"
MESH = pl.DeviceIdType.MESH
TILE = 16
CHUNK = 8
GROUPS = 4
NEAR = 2


def rows_cols(n_rows, n_cols):
    shape = (n_rows, n_cols)
    return lax.broadcasted_iota(jnp.int32, shape, 0), lax.broadcasted_iota(jnp.int32, shape, 1)


def banded(tap, n_taps, tap_index, valid):
    index = jnp.where(valid, tap_index, -1)
    total = jnp.zeros(index.shape, jnp.float32)
    for t in range(n_taps):
        total = jnp.where(index == t, tap(t), total)
    return total.astype(jnp.bfloat16)


def x_matrix(tap, n_taps, last_tile):
    half = (n_taps - 1) // 2
    own = CHUNK * TILE
    r, k = rows_cols(own + CHUNK * half, (CHUNK + 2 * half) * TILE)
    s = jnp.maximum(r - own, 0)
    plane = jnp.where(r < own, r // TILE, s // half)
    row = jnp.where(r < own, r % TILE, s % half + (TILE - half if last_tile else 0))
    return banded(tap, n_taps, k // TILE - plane, row == k % TILE)


def y_matrix(tap, n_taps, extent):
    half = (n_taps - 1) // 2
    own, slab = CHUNK * extent, CHUNK * half
    r, k = rows_cols(own, own + 2 * slab)
    s = jnp.maximum(jnp.where(k < own + slab, k - own, k - own - slab), 0)
    plane = jnp.where(k < own, k // extent, s // half)
    pos = jnp.where(k < own, k % extent + half, jnp.where(k < own + slab, s % half, s % half + half + extent))
    return banded(tap, n_taps, pos - r % extent, plane == r // extent)


def z_matrix(tap, n_taps, depth):
    r, k = rows_cols(2 * depth, 2 * depth)
    return banded(tap, n_taps, r % depth - k % depth + (n_taps - 1) // 2, r // depth == k // depth)


def mix_matrix(weight):
    n = weight.shape[0]
    r, k = rows_cols(n, n * TILE)
    across = (k // TILE == r).astype(jnp.bfloat16)
    m, c = rows_cols(n * TILE, n)
    along = (m // TILE == c).astype(jnp.bfloat16)
    wide = jnp.dot(weight.T, across, preferred_element_type=jnp.float32).astype(jnp.bfloat16)
    full = jnp.dot(along, wide, preferred_element_type=jnp.float32)
    m, k = rows_cols(n * TILE, n * TILE)
    return jnp.where(m % TILE == k % TILE, full, 0.0).astype(jnp.bfloat16)


def matrices_kernel(taps, weights, bias_col, ax0, ax1, ay, bz, wk, bias):
    n_taps = taps.shape[2]
    layer = pl.program_id(0)
    extent = ay.shape[1] // CHUNK
    ax0[0] = x_matrix(lambda t: taps[layer, 0, t], n_taps, False)
    ax1[0] = x_matrix(lambda t: taps[layer, 0, t], n_taps, True)
    ay[0] = y_matrix(lambda t: taps[layer, 1, t], n_taps, extent)
    bz[0] = z_matrix(lambda t: taps[layer, 2, t], n_taps, bz.shape[1] // 2)
    wk[0] = mix_matrix(weights[0])
    n = weights.shape[1]
    m, c = rows_cols(n * TILE, n)
    spread = jnp.sum(jnp.where(m // TILE == c, bias_col[0], 0.0), axis=1, keepdims=True)
    bias[0] = jnp.broadcast_to(spread, bias.shape[1:])


def matrices(filter_taps, mix_weights, mix_bias, extent, depth):
    layers, _, n_taps = filter_taps.shape
    chans = mix_weights.shape[1]
    half = (n_taps - 1) // 2
    taps = lax.reduce_precision(filter_taps, 8, 7)
    own_x, own_y = CHUNK * TILE, CHUNK * extent
    slab = CHUNK * half
    shapes = [(own_x + slab, own_x + 2 * half * TILE)] * 2
    shapes += [(own_y, own_y + 2 * slab), (2 * depth, 2 * depth), (chans * TILE, chans * TILE)]
    outs = [jax.ShapeDtypeStruct((layers,) + s, jnp.bfloat16) for s in shapes]
    outs.append(jax.ShapeDtypeStruct((layers, chans * TILE, depth), jnp.float32))
    return pl.pallas_call(
        matrices_kernel, grid=(layers,), out_shape=outs,
        in_specs=[pl.BlockSpec(memory_space=pltpu.SMEM), pl.BlockSpec((1, chans, chans), lambda i: (i, 0, 0)),
                  pl.BlockSpec((1, 1, chans), lambda i: (i, 0, 0))],
        out_specs=[pl.BlockSpec((1,) + o.shape[1:], lambda i: (i, 0, 0)) for o in outs],
        name="matrices",
    )(taps, mix_weights, mix_bias[:, None, :])


def gelu(v):
    c0 = 0.7978845608028654
    arg = v * (c0 + (c0 * 0.044715) * (v * v))
    h = 0.5 * v
    return h + h * jnp.tanh(arg)


def layer_kernel(layer, nx, ny, half, v_hbm, ax0_hbm, ax1_hbm, ay_hbm, bz_hbm, wk_hbm, bias_hbm, out_hbm,
                 vext, u1, send, recv, stage, ax, ay, bz, wk, bias,
                 load_sem, const_sem, xsend, xrecv, ysend, yrecv, out_sem):
    chans, planes, extent, depth = u1.shape
    n_chunks = planes // CHUNK
    per_group = chans // GROUPS
    far = half - NEAR
    slab = CHUNK * half
    window = CHUNK + 2 * half
    bi, yi, xi = lax.axis_index(PARTS_AXIS), lax.axis_index(COL_AXIS), lax.axis_index(ROW_AXIS)
    left = (bi, yi, lax.rem(xi + nx - 1, nx))
    right = (bi, yi, lax.rem(xi + 1, nx))
    up = (bi, lax.rem(yi + ny - 1, ny), xi)
    down = (bi, lax.rem(yi + 1, ny), xi)
    has_left, has_right, has_up, has_down = xi > 0, xi < nx - 1, yi > 0, yi < ny - 1

    def load(g):
        cs = pl.ds(g * per_group, per_group)
        return pltpu.make_async_copy(v_hbm.at[cs], vext.at[cs, pl.ds(half, planes)], load_sem.at[g])

    consts = [pltpu.make_async_copy(src.at[layer], dst, const_sem.at[i]) for i, (src, dst) in enumerate(
        ((ax0_hbm, ax.at[0]), (ax1_hbm, ax.at[1]), (ay_hbm, ay), (bz_hbm, bz), (wk_hbm, wk), (bias_hbm, bias)))]
    for c in consts:
        c.start()
    for g in range(GROUPS):
        load(g).start()

    barrier = pltpu.get_barrier_semaphore()
    for dev in (left, right, up, down):
        pl.semaphore_signal(barrier, inc=1, device_id=dev, device_id_type=MESH)
    pl.semaphore_wait(barrier, 4)

    def x_copy(to_right, is_far, g):
        cs = pl.ds(g * per_group, per_group)
        if to_right:
            src, dst, n = (planes - half, 0, far) if is_far else (planes - NEAR, half - NEAR, NEAR)
        else:
            src, dst, n = (NEAR, half + planes + NEAR, far) if is_far else (0, half + planes, NEAR)
        d, f = int(to_right), int(is_far)
        return pltpu.make_async_remote_copy(
            src_ref=v_hbm.at[cs, pl.ds(src, n)], dst_ref=vext.at[cs, pl.ds(dst, n)],
            send_sem=xsend.at[d, f, g], recv_sem=xrecv.at[d, f, g],
            device_id=right if to_right else left, device_id_type=MESH)

    for is_far in (False, True):
        for g in range(GROUPS):
            @pl.when(has_right)
            def _():
                x_copy(True, is_far, g).start()

            @pl.when(has_left)
            def _():
                x_copy(False, is_far, g).start()

    def fill_x(start):
        @pl.loop(0, chans)
        def _(c):
            vext[c, pl.ds(start, half)] = jnp.zeros((half, extent, depth), jnp.bfloat16)

    def fill_y(side):
        @pl.loop(0, chans)
        def _(c):
            for j in range(n_chunks):
                recv[j, side, c] = jnp.zeros((slab, depth), jnp.bfloat16)

    @pl.when(jnp.logical_not(has_left))
    def _():
        fill_x(0)

    @pl.when(jnp.logical_not(has_right))
    def _():
        fill_x(half + planes)

    @pl.when(jnp.logical_not(has_up))
    def _():
        fill_y(0)

    @pl.when(jnp.logical_not(has_down))
    def _():
        fill_y(1)

    for c in consts:
        c.wait()

    def y_copy(j, slot, side, cs):
        return pltpu.make_async_remote_copy(
            src_ref=send.at[slot, side, cs], dst_ref=recv.at[j, 1 - side, cs],
            send_sem=ysend.at[slot, side], recv_sem=yrecv.at[j, 1 - side],
            device_id=down if side else up, device_id_type=MESH)

    every = pl.ds(0, chans)

    def wait_sent(j, slot):
        @pl.when(has_up)
        def _():
            y_copy(j, slot, 0, every).wait_send()

        @pl.when(has_down)
        def _():
            y_copy(j, slot, 1, every).wait_send()

    def x_pass(j, slot, waits):
        own = CHUNK * TILE

        @pl.loop(0, GROUPS)
        def _(g):
            for cond, copy in waits:
                if cond is None:
                    copy(g).wait()
                else:
                    @pl.when(cond)
                    def _():
                        copy(g).wait_recv()

            @pl.loop(0, per_group // 2)
            def _(p):
                c = g * per_group + 2 * p
                for t in range(2):
                    pair = [vext[c + i, pl.ds(j * CHUNK, window), pl.ds(t * TILE, TILE)].reshape(window * TILE, depth)
                            for i in range(2)]
                    got = jnp.dot(ax[t], jnp.concatenate(pair, axis=1), preferred_element_type=jnp.float32)
                    got = got.astype(jnp.bfloat16)
                    for i in range(2):
                        part = got[:, i * depth:(i + 1) * depth]
                        u1[c + i, pl.ds(j * CHUNK, CHUNK), pl.ds(t * TILE, TILE)] = part[:own].reshape(CHUNK, TILE, depth)
                        send[slot, t, c + i] = part[own:]

            cs = pl.ds(g * per_group, per_group)

            @pl.when(has_up)
            def _():
                y_copy(j, slot, 0, cs).start()

            @pl.when(has_down)
            def _():
                y_copy(j, slot, 1, cs).start()

    def out_copy(s, x):
        return pltpu.make_async_copy(stage.at[s], out_hbm.at[:, x], out_sem.at[s])

    def yz_mix(j, first):
        slot = 0

        @pl.when(has_up)
        def _():
            y_copy(j, slot, 1, every).wait_recv()

        @pl.when(has_down)
        def _():
            y_copy(j, slot, 0, every).wait_recv()

        chunk = pl.ds(j * CHUNK, CHUNK)

        @pl.loop(0, chans // 4)
        def _(q):
            for h in range(2):
                c = 4 * q + 2 * h
                own = jnp.concatenate([u1[c + i, chunk].reshape(CHUNK * extent, depth) for i in range(2)], axis=1)
                top = jnp.concatenate([recv[j, 0, c + i] for i in range(2)], axis=1)
                bot = jnp.concatenate([recv[j, 1, c + i] for i in range(2)], axis=1)
                rhs = jnp.concatenate([own, top, bot], axis=0)
                u2 = jnp.dot(ay[...], rhs, preferred_element_type=jnp.float32).astype(jnp.bfloat16)
                u3 = jnp.dot(u2, bz[...], preferred_element_type=jnp.float32).astype(jnp.bfloat16)
                for i in range(2):
                    u1[c + i, chunk] = u3[:, i * depth:(i + 1) * depth].reshape(CHUNK, extent, depth)

        @pl.loop(0, CHUNK // 2)
        def _(i):
            for s in range(2):
                x = j * CHUNK + 2 * i + s
                if first:
                    @pl.when(i > 0)
                    def _():
                        out_copy(s, x).wait()
                else:
                    out_copy(s, x).wait()
                rhs = jnp.concatenate(
                    [u1[:, x, pl.ds(t * TILE, TILE)].reshape(chans * TILE, depth) for t in range(2)], axis=1)
                step = 256
                for m in range(chans * TILE // step):
                    acc = jnp.dot(wk[pl.ds(m * step, step)], rhs, preferred_element_type=jnp.float32)
                    cs = pl.ds(m * (step // TILE), step // TILE)
                    for t in range(2):
                        pre = acc[:, t * depth:(t + 1) * depth] + bias[pl.ds(m * step, step)]
                        old = vext[cs, half + x, pl.ds(t * TILE, TILE)].reshape(step, depth).astype(jnp.float32)
                        new = (old + gelu(pre)).astype(jnp.bfloat16)
                        stage[s, cs, pl.ds(t * TILE, TILE)] = new.reshape(step // TILE, TILE, depth)
                out_copy(s, x).start()

    from_left = (has_left, lambda g: x_copy(True, False, g))
    from_right = (has_right, lambda g: x_copy(False, False, g))
    far_left = (has_left, lambda g: x_copy(True, True, g))
    far_right = (has_right, lambda g: x_copy(False, True, g))

    x_pass(1, 0, [(None, load), from_left])
    x_pass(2, 1, [from_right])
    yz_mix(1, True)
    wait_sent(1, 0)
    x_pass(0, 0, [far_left])
    wait_sent(2, 1)
    x_pass(3, 1, [far_right])

    @pl.loop(0, 3)
    def _(k):
        yz_mix(lax.rem(2 + 3 * k, 5), False)

    wait_sent(0, 0)
    wait_sent(3, 1)
    for is_far in (False, True):
        for g in range(GROUPS):
            @pl.when(has_right)
            def _():
                x_copy(True, is_far, g).wait_send()

            @pl.when(has_left)
            def _():
                x_copy(False, is_far, g).wait_send()
    for s in range(2):
        out_copy(s, s).wait()


def solution(mesh):
    nx, ny = mesh.shape[ROW_AXIS], mesh.shape[COL_AXIS]
    vol_spec = P(PARTS_AXIS, ROW_AXIS, COL_AXIS, None)

    def local_layers(volume, filter_taps, mix_weights, mix_bias):
        chans, planes, extent, depth = volume.shape
        half = (filter_taps.shape[2] - 1) // 2
        slab = CHUNK * half
        mats = matrices(filter_taps, mix_weights, mix_bias, extent, depth)
        bf = jnp.bfloat16
        current = volume
        for layer in range(filter_taps.shape[0]):
            current = pl.pallas_call(
                functools.partial(layer_kernel, layer, nx, ny, half),
                out_shape=jax.ShapeDtypeStruct(volume.shape, bf),
                in_specs=[pl.BlockSpec(memory_space=pl.ANY)] * 7,
                out_specs=pl.BlockSpec(memory_space=pl.ANY),
                scratch_shapes=[
                    pltpu.VMEM((chans, planes + 2 * half, extent, depth), bf),
                    pltpu.VMEM(volume.shape, bf),
                    pltpu.VMEM((2, 2, chans, slab, depth), bf),
                    pltpu.VMEM((planes // CHUNK, 2, chans, slab, depth), bf),
                    pltpu.VMEM((2, chans, extent, depth), bf),
                    pltpu.VMEM((2,) + mats[0].shape[1:], bf),
                    pltpu.VMEM(mats[2].shape[1:], bf),
                    pltpu.VMEM(mats[3].shape[1:], bf),
                    pltpu.VMEM(mats[4].shape[1:], bf),
                    pltpu.VMEM(mats[5].shape[1:], jnp.float32),
                    pltpu.SemaphoreType.DMA((GROUPS,)),
                    pltpu.SemaphoreType.DMA((6,)),
                    pltpu.SemaphoreType.DMA((2, 2, GROUPS)),
                    pltpu.SemaphoreType.DMA((2, 2, GROUPS)),
                    pltpu.SemaphoreType.DMA((2, 2)),
                    pltpu.SemaphoreType.DMA((planes // CHUNK, 2)),
                    pltpu.SemaphoreType.DMA((2,)),
                ],
                compiler_params=pltpu.CompilerParams(
                    collective_id=layer, has_side_effects=True, vmem_limit_bytes=67043328),
                name=f"layer_{layer}",
            )(current, *mats)
        return current

    return jax.shard_map(local_layers, mesh=mesh, in_specs=(vol_spec, P(), P(), P()), out_specs=vol_spec, check_vma=False)
```

```python
import functools

import jax
import jax.numpy as jnp
from jax import lax
from jax.experimental import pallas as pl
from jax.experimental.pallas import tpu as pltpu
from jax.sharding import PartitionSpec as P

PARTS_AXIS = "batch"
COL_AXIS = "ysp"
ROW_AXIS = "xsp"
MESH = pl.DeviceIdType.MESH
TILE = 16
CHUNK = 4
GROUPS = 4
SLOTS = 5


def rows_cols(n_rows, n_cols):
    shape = (n_rows, n_cols)
    return lax.broadcasted_iota(jnp.int32, shape, 0), lax.broadcasted_iota(jnp.int32, shape, 1)


def banded(tap, n_taps, tap_index, valid):
    index = jnp.where(valid, tap_index, -1)
    total = jnp.zeros(index.shape, jnp.float32)
    for t in range(n_taps):
        total = jnp.where(index == t, tap(t), total)
    return total.astype(jnp.bfloat16)


def x_matrix(tap, n_taps, last_tile):
    half = (n_taps - 1) // 2
    own = CHUNK * TILE
    r, k = rows_cols(own + CHUNK * half, (CHUNK + 2 * half) * TILE)
    s = jnp.maximum(r - own, 0)
    plane = jnp.where(r < own, r // TILE, s // half)
    row = jnp.where(r < own, r % TILE, s % half + (TILE - half if last_tile else 0))
    return banded(tap, n_taps, k // TILE - plane, row == k % TILE)


def y_matrix(tap, n_taps, extent):
    half = (n_taps - 1) // 2
    own, slab = CHUNK * extent, CHUNK * half
    r, k = rows_cols(own, own + 2 * slab)
    s = jnp.maximum(jnp.where(k < own + slab, k - own, k - own - slab), 0)
    plane = jnp.where(k < own, k // extent, s // half)
    pos = jnp.where(k < own, k % extent + half, jnp.where(k < own + slab, s % half, s % half + half + extent))
    return banded(tap, n_taps, pos - r % extent, plane == r // extent)


def z_matrix(tap, n_taps, depth):
    r, k = rows_cols(2 * depth, 2 * depth)
    return banded(tap, n_taps, r % depth - k % depth + (n_taps - 1) // 2, r // depth == k // depth)


def gelu(v):
    c0 = 0.7978845608028654
    arg = v * (c0 + (c0 * 0.044715) * (v * v))
    h = 0.5 * v
    return h + h * jnp.tanh(arg)


def stack_kernel(nx, ny, v_hbm, taps, weights, biases, out_hbm, vext, u1, send, recv, ax, ay, bz, wk, bias,
                 load_sem, xsend, xrecv, ysend, yrecv, out_sem, ycred, xcred):
    chans, planes, extent, depth = u1.shape
    n_layers, _, n_taps = taps.shape
    half = (n_taps - 1) // 2
    n_chunks = planes // CHUNK
    middle = n_chunks // 2
    per_group = chans // GROUPS
    slab = CHUNK * half
    window = CHUNK + 2 * half
    near = half - 2 * CHUNK
    bi, yi, xi = lax.axis_index(PARTS_AXIS), lax.axis_index(COL_AXIS), lax.axis_index(ROW_AXIS)
    left = (bi, yi, lax.rem(xi + nx - 1, nx))
    right = (bi, yi, lax.rem(xi + 1, nx))
    up = (bi, lax.rem(yi + ny - 1, ny), xi)
    down = (bi, lax.rem(yi + 1, ny), xi)
    has_left, has_right, has_up, has_down = xi > 0, xi < nx - 1, yi > 0, yi < ny - 1
    beside = ((has_left, left), (has_right, right))
    above = ((has_up, up), (has_down, down))

    def chunk_of(n):
        low = middle - 1 - n // 2
        return low + (n % 2) * (1 + 2 * (n // 2))

    def load(g):
        cs = pl.ds(g * per_group, per_group)
        return pltpu.make_async_copy(v_hbm.at[cs], vext.at[cs, pl.ds(half, planes)], load_sem.at[g])

    pieces = ((0, near), (near, CHUNK - near), (CHUNK, CHUNK), (2 * CHUNK, near))

    def x_copy(side, piece, layer):
        first, n = pieces[piece]
        src = planes - first - n if side else first
        dst = src + half - planes if side else src + half + planes
        source = v_hbm.at[:, pl.ds(src, n)] if layer == 0 else vext.at[:, pl.ds(half + src, n)]
        return pltpu.make_async_remote_copy(
            src_ref=source, dst_ref=vext.at[:, pl.ds(dst, n)],
            send_sem=xsend.at[side, piece], recv_sem=xrecv.at[side, piece],
            device_id=beside[side][1], device_id_type=MESH)

    def x_start(side, which, layer):
        @pl.when(beside[side][0])
        def _():
            for piece in which:
                x_copy(side, piece, layer).start()

    def y_copy(k, slot, side, g):
        cs = pl.ds(g * per_group, per_group)
        return pltpu.make_async_remote_copy(
            src_ref=send.at[slot, side, cs], dst_ref=recv.at[k, cs, pl.ds((1 - side) * slab, slab)],
            send_sem=ysend.at[slot, side, g], recv_sem=yrecv.at[k, 1 - side, g],
            device_id=above[side][1], device_id_type=MESH)

    def set_x_matrices(layer):
        for t in range(2):
            ax[t] = x_matrix(lambda i: taps[layer, 0, i], n_taps, t == 1)

    def set_other_matrices(layer):
        ay[...] = y_matrix(lambda i: taps[layer, 1, i], n_taps, extent)
        bz[...] = z_matrix(lambda i: taps[layer, 2, i], n_taps, depth)
        block = 128

        @pl.loop(0, chans * TILE // block)
        def _(b):
            r, k = rows_cols(chans, chans * TILE)
            across = (k // TILE == r).astype(jnp.bfloat16)
            wide = jnp.dot(weights[layer].T, across, preferred_element_type=jnp.float32).astype(jnp.bfloat16)
            m, c = rows_cols(block, chans)
            mine = (m + b * block) // TILE == c
            full = jnp.dot(mine.astype(jnp.bfloat16), wide, preferred_element_type=jnp.float32)
            m, k = rows_cols(block, chans * TILE)
            at = pl.ds(pl.multiple_of(b * block, block), block)
            wk[at] = jnp.where(m % TILE == k % TILE, full, 0.0).astype(jnp.bfloat16)
            spread = jnp.sum(jnp.where(mine, biases[pl.ds(layer, 1)], 0.0), axis=1, keepdims=True)
            bias[at] = jnp.broadcast_to(spread, (block, depth))

    def x_pass(layer, n):
        k = chunk_of(n)
        own = CHUNK * TILE
        turn = n_chunks * layer + n
        slot = turn % SLOTS
        side = n % 2
        reach = {1: (0,), 2: (1, 2), 3: (3,)}.get(n // 2, ())
        if reach:
            @pl.when(beside[side][0])
            def _():
                for piece in reach:
                    x_copy(1 - side, piece, layer).wait_recv()
        for s in range(2):
            @pl.when(above[s][0])
            def _():
                if turn >= SLOTS:
                    for g in range(GROUPS):
                        y_copy(chunk_of((turn - SLOTS) % n_chunks), slot, s, g).wait_send()
                if layer > 0:
                    pl.semaphore_wait(ycred.at[s], 1)

        @pl.loop(0, GROUPS)
        def _(g):
            if turn == 0:
                load(g).wait()

            @pl.loop(0, per_group // 2)
            def _(p):
                c = g * per_group + 2 * p
                for t in range(2):
                    pair = [vext[c + i, pl.ds(k * CHUNK, window), pl.ds(t * TILE, TILE)].reshape(window * TILE, depth)
                            for i in range(2)]
                    got = jnp.dot(ax[t], jnp.concatenate(pair, axis=1), preferred_element_type=jnp.float32)
                    got = got.astype(jnp.bfloat16)
                    for i in range(2):
                        part = got[:, i * depth:(i + 1) * depth]
                        u1[c + i, pl.ds(k * CHUNK, CHUNK), pl.ds(t * TILE, TILE)] = part[:own].reshape(CHUNK, TILE, depth)
                        send[slot, t, c + i] = part[own:]

            for s in range(2):
                @pl.when(above[s][0])
                def _():
                    y_copy(k, slot, s, g).start()

        if n >= n_chunks - 2 and layer < n_layers - 1:
            @pl.when(beside[side][0])
            def _():
                pl.semaphore_signal(xcred.at[1 - side], inc=1, device_id=beside[side][1], device_id_type=MESH)

    def out_copy(k):
        return pltpu.make_async_copy(
            vext.at[:, pl.ds(half + k * CHUNK, CHUNK)], out_hbm.at[:, pl.ds(k * CHUNK, CHUNK)], out_sem.at[k])

    def yz_mix(layer, n):
        k = chunk_of(n)
        chunk = pl.ds(k * CHUNK, CHUNK)

        @pl.loop(0, GROUPS)
        def _(g):
            for s in range(2):
                @pl.when(above[1 - s][0])
                def _():
                    y_copy(k, 0, s, g).wait_recv()

            @pl.loop(0, per_group // 8)
            def _(q):
                for h in range(4):
                    c = g * per_group + 8 * q + 2 * h
                    own = jnp.concatenate([u1[c + i, chunk].reshape(CHUNK * extent, depth) for i in range(2)], axis=1)
                    halo = jnp.concatenate([recv[k, c + i] for i in range(2)], axis=1)
                    rhs = jnp.concatenate([own, halo], axis=0)
                    u2 = jnp.dot(ay[...], rhs, preferred_element_type=jnp.float32).astype(jnp.bfloat16)
                    u3 = jnp.dot(u2, bz[...], preferred_element_type=jnp.float32).astype(jnp.bfloat16)
                    for i in range(2):
                        u1[c + i, chunk] = u3[:, i * depth:(i + 1) * depth].reshape(CHUNK, extent, depth)

        if layer < n_layers - 1:
            for s in range(2):
                @pl.when(above[s][0])
                def _():
                    pl.semaphore_signal(ycred.at[1 - s], inc=1, device_id=above[s][1], device_id_type=MESH)

        @pl.loop(0, CHUNK // 2)
        def _(i):
            for s in range(2):
                x = k * CHUNK + 2 * i + s
                rhs = jnp.concatenate(
                    [u1[:, x, pl.ds(t * TILE, TILE)].reshape(chans * TILE, depth) for t in range(2)], axis=1)
                step = 256
                for m in range(chans * TILE // step):
                    acc = jnp.dot(wk[pl.ds(m * step, step)], rhs, preferred_element_type=jnp.float32)
                    cs = pl.ds(m * (step // TILE), step // TILE)
                    for t in range(2):
                        at = (cs, half + x, pl.ds(t * TILE, TILE))
                        pre = acc[:, t * depth:(t + 1) * depth] + bias[pl.ds(m * step, step)]
                        old = vext[at].reshape(step, depth).astype(jnp.float32)
                        vext[at] = (old + gelu(pre)).astype(jnp.bfloat16).reshape(step // TILE, TILE, depth)

        if layer == n_layers - 1:
            out_copy(k).start()

    def send_halo(layer, n):
        side, which = n % 2, {1: (3,), 2: (2,), 3: (0, 1)}[n // 2]
        if n // 2 == 1:
            @pl.when(beside[side][0])
            def _():
                pl.semaphore_wait(xcred.at[side], 1)
        x_start(side, which, layer + 1)

    for g in range(GROUPS):
        load(g).start()
    barrier = pltpu.get_barrier_semaphore()
    for dev in (left, right, up, down):
        pl.semaphore_signal(barrier, inc=1, device_id=dev, device_id_type=MESH)
    pl.semaphore_wait(barrier, 4)
    for piece in range(4):
        for side in range(2):
            x_start(side, (piece,), 0)
    set_x_matrices(0)
    x_pass(0, 0)

    for side in range(2):
        @pl.when(jnp.logical_not(beside[side][0]))
        def _():
            @pl.loop(0, chans)
            def _(c):
                vext[c, pl.ds(side * (half + planes), half)] = jnp.zeros((half, extent, depth), jnp.bfloat16)

        @pl.when(jnp.logical_not(above[side][0]))
        def _():
            @pl.loop(0, chans)
            def _(c):
                for k in range(n_chunks):
                    recv[k, c, pl.ds(side * slab, slab)] = jnp.zeros((slab, depth), jnp.bfloat16)

    last = n_chunks - 1
    for layer in range(n_layers):
        for n in range(1, n_chunks):
            x_pass(layer, n)
        for side in range(2):
            @pl.when(beside[side][0])
            def _():
                for piece in range(4):
                    x_copy(side, piece, layer).wait_send()
        if layer < n_layers - 1:
            set_x_matrices(layer + 1)
        set_other_matrices(layer)

        @pl.loop(0, last)
        def _(n):
            yz_mix(layer, n)
            if layer < n_layers - 1:
                for m in range(2, last):
                    @pl.when(n == m)
                    def _():
                        send_halo(layer, m)

        if layer < n_layers - 1:
            x_pass(layer + 1, 0)
        yz_mix(layer, last)
        if layer < n_layers - 1:
            send_halo(layer, last)

    turns = n_chunks * n_layers
    for turn in range(max(0, turns - SLOTS), turns):
        for s in range(2):
            @pl.when(above[s][0])
            def _():
                for g in range(GROUPS):
                    y_copy(chunk_of(turn % n_chunks), turn % SLOTS, s, g).wait_send()
    for k in range(n_chunks):
        out_copy(k).wait()


def solution(mesh):
    nx, ny = mesh.shape[ROW_AXIS], mesh.shape[COL_AXIS]
    vol_spec = P(PARTS_AXIS, ROW_AXIS, COL_AXIS, None)

    def local_layers(volume, filter_taps, mix_weights, mix_bias):
        chans, planes, extent, depth = volume.shape
        half = (filter_taps.shape[2] - 1) // 2
        n_chunks, slab = planes // CHUNK, CHUNK * half
        bf = jnp.bfloat16
        return pl.pallas_call(
            functools.partial(stack_kernel, nx, ny),
            out_shape=jax.ShapeDtypeStruct(volume.shape, bf),
            in_specs=[pl.BlockSpec(memory_space=pl.ANY), pl.BlockSpec(memory_space=pltpu.SMEM),
                      pl.BlockSpec(memory_space=pltpu.VMEM), pl.BlockSpec(memory_space=pltpu.VMEM)],
            out_specs=pl.BlockSpec(memory_space=pl.ANY),
            scratch_shapes=[
                pltpu.VMEM((chans, planes + 2 * half, extent, depth), bf),
                pltpu.VMEM(volume.shape, bf),
                pltpu.VMEM((SLOTS, 2, chans, slab, depth), bf),
                pltpu.VMEM((n_chunks, chans, 2 * slab, depth), bf),
                pltpu.VMEM((2, CHUNK * TILE + slab, (CHUNK + 2 * half) * TILE), bf),
                pltpu.VMEM((CHUNK * extent, CHUNK * extent + 2 * slab), bf),
                pltpu.VMEM((2 * depth, 2 * depth), bf),
                pltpu.VMEM((chans * TILE, chans * TILE), bf),
                pltpu.VMEM((chans * TILE, depth), jnp.float32),
                pltpu.SemaphoreType.DMA((GROUPS,)),
                pltpu.SemaphoreType.DMA((2, 4)),
                pltpu.SemaphoreType.DMA((2, 4)),
                pltpu.SemaphoreType.DMA((SLOTS, 2, GROUPS)),
                pltpu.SemaphoreType.DMA((n_chunks, 2, GROUPS)),
                pltpu.SemaphoreType.DMA((n_chunks,)),
                pltpu.SemaphoreType.REGULAR((2,)),
                pltpu.SemaphoreType.REGULAR((2,)),
            ],
            compiler_params=pltpu.CompilerParams(
                collective_id=0, has_side_effects=True, vmem_limit_bytes=67043328),
            name="stack",
        )(volume, filter_taps, mix_weights, mix_bias)

    return jax.shard_map(local_layers, mesh=mesh, in_specs=(vol_spec, P(), P(), P()), out_specs=vol_spec, check_vma=False)
```

```python
import functools

import jax
import jax.numpy as jnp
from jax import lax
from jax.experimental import pallas as pl
from jax.experimental.pallas import tpu as pltpu
from jax.sharding import PartitionSpec as P

PARTS_AXIS = "batch"
COL_AXIS = "ysp"
ROW_AXIS = "xsp"
MESH = pl.DeviceIdType.MESH
TILE = 16
CHUNK = 4
GROUPS = 4
SLOTS = 5


def rows_cols(n_rows, n_cols):
    shape = (n_rows, n_cols)
    return lax.broadcasted_iota(jnp.int32, shape, 0), lax.broadcasted_iota(jnp.int32, shape, 1)


def banded(tap, n_taps, tap_index, valid):
    index = jnp.where(valid, tap_index, -1)
    total = jnp.zeros(index.shape, jnp.float32)
    for t in range(n_taps):
        total = jnp.where(index == t, tap(t), total)
    return total.astype(jnp.bfloat16)


def x_matrix(tap, n_taps, last_tile):
    half = (n_taps - 1) // 2
    own = CHUNK * TILE
    r, k = rows_cols(own + CHUNK * half, (CHUNK + 2 * half) * TILE)
    s = jnp.maximum(r - own, 0)
    plane = jnp.where(r < own, r // TILE, s // half)
    row = jnp.where(r < own, r % TILE, s % half + (TILE - half if last_tile else 0))
    return banded(tap, n_taps, k // TILE - plane, row == k % TILE)


def y_matrix(tap, n_taps, extent):
    half = (n_taps - 1) // 2
    own, slab = CHUNK * extent, CHUNK * half
    r, k = rows_cols(own, own + 2 * slab)
    s = jnp.maximum(jnp.where(k < own + slab, k - own, k - own - slab), 0)
    plane = jnp.where(k < own, k // extent, s // half)
    pos = jnp.where(k < own, k % extent + half, jnp.where(k < own + slab, s % half, s % half + half + extent))
    return banded(tap, n_taps, pos - r % extent, plane == r // extent)


def z_matrix(tap, n_taps, depth):
    r, k = rows_cols(2 * depth, 2 * depth)
    return banded(tap, n_taps, r % depth - k % depth + (n_taps - 1) // 2, r // depth == k // depth)


def gelu(v):
    c0 = 0.7978845608028654
    arg = v * (c0 + (c0 * 0.044715) * (v * v))
    h = 0.5 * v
    return h + h * jnp.tanh(arg)


def stack_kernel(nx, ny, v_hbm, taps, weights, biases, u1, vext, send, recv, ax, ay, bz, wk, bias,
                 load_sem, xsend, xrecv, ysend, yrecv, ycred, xcred):
    chans, planes, extent, depth = u1.shape
    n_layers, _, n_taps = taps.shape
    half = (n_taps - 1) // 2
    n_chunks = planes // CHUNK
    middle = n_chunks // 2
    per_group = chans // GROUPS
    slab = CHUNK * half
    window = CHUNK + 2 * half
    near = half - 2 * CHUNK
    bi, yi, xi = lax.axis_index(PARTS_AXIS), lax.axis_index(COL_AXIS), lax.axis_index(ROW_AXIS)
    left = (bi, yi, lax.rem(xi + nx - 1, nx))
    right = (bi, yi, lax.rem(xi + 1, nx))
    up = (bi, lax.rem(yi + ny - 1, ny), xi)
    down = (bi, lax.rem(yi + 1, ny), xi)
    has_left, has_right, has_up, has_down = xi > 0, xi < nx - 1, yi > 0, yi < ny - 1
    beside = ((has_left, left), (has_right, right))
    above = ((has_up, up), (has_down, down))

    def side_of(n):
        m, b = n // 2, n % 2
        swap = m * (middle - 1 - m) // 2
        return b + swap - 2 * b * swap

    def chunk_of(n):
        return middle - 1 - n // 2 + side_of(n) * (1 + 2 * (n // 2))

    def load(g):
        cs = pl.ds(g * per_group, per_group)
        return pltpu.make_async_copy(v_hbm.at[cs], vext.at[cs, pl.ds(half, planes)], load_sem.at[g])

    pieces = ((0, near), (near, CHUNK - near), (CHUNK, CHUNK), (2 * CHUNK, near))

    def x_copy(side, piece, layer):
        first, n = pieces[piece]
        src = planes - first - n if side else first
        dst = src + half - planes if side else src + half + planes
        source = v_hbm.at[:, pl.ds(src, n)] if layer == 0 else vext.at[:, pl.ds(half + src, n)]
        return pltpu.make_async_remote_copy(
            src_ref=source, dst_ref=vext.at[:, pl.ds(dst, n)],
            send_sem=xsend.at[side, piece], recv_sem=xrecv.at[side, piece],
            device_id=beside[side][1], device_id_type=MESH)

    def x_start(side, which, layer):
        @pl.when(beside[side][0])
        def _():
            for piece in which:
                x_copy(side, piece, layer).start()

    def y_copy(k, slot, side, g):
        cs = pl.ds(g * per_group, per_group)
        return pltpu.make_async_remote_copy(
            src_ref=send.at[slot, side, cs], dst_ref=recv.at[k, cs, pl.ds((1 - side) * slab, slab)],
            send_sem=ysend.at[slot, side, g], recv_sem=yrecv.at[k, 1 - side, g],
            device_id=above[side][1], device_id_type=MESH)

    def set_x_matrices(layer):
        for t in range(2):
            ax[t] = x_matrix(lambda i: taps[layer, 0, i], n_taps, t == 1)

    def set_other_matrices(layer):
        ay[...] = y_matrix(lambda i: taps[layer, 1, i], n_taps, extent)
        bz[...] = z_matrix(lambda i: taps[layer, 2, i], n_taps, depth)
        block = 128

        @pl.loop(0, chans * TILE // block)
        def _(b):
            r, k = rows_cols(chans, chans * TILE)
            across = (k // TILE == r).astype(jnp.bfloat16)
            wide = jnp.dot(weights[layer].T, across, preferred_element_type=jnp.float32).astype(jnp.bfloat16)
            m, c = rows_cols(block, chans)
            mine = (m + b * block) // TILE == c
            full = jnp.dot(mine.astype(jnp.bfloat16), wide, preferred_element_type=jnp.float32)
            m, k = rows_cols(block, chans * TILE)
            at = pl.ds(pl.multiple_of(b * block, block), block)
            wk[at] = jnp.where(m % TILE == k % TILE, full, 0.0).astype(jnp.bfloat16)
            spread = jnp.sum(jnp.where(mine, biases[pl.ds(layer, 1)], 0.0), axis=1, keepdims=True)
            bias[at] = jnp.broadcast_to(spread, (block, depth))

    def x_pass(layer, n):
        k = chunk_of(n)
        own = CHUNK * TILE
        turn = n_chunks * layer + n
        slot = turn % SLOTS
        side = side_of(n)
        reach = {1: (0,), 2: (1, 2), 3: (3,)}.get(n // 2, ())
        if reach:
            @pl.when(beside[side][0])
            def _():
                for piece in reach:
                    x_copy(1 - side, piece, layer).wait_recv()
        for s in range(2):
            @pl.when(above[s][0])
            def _():
                if turn >= SLOTS:
                    for g in range(GROUPS):
                        y_copy(chunk_of((turn - SLOTS) % n_chunks), slot, s, g).wait_send()
                if layer > 0:
                    pl.semaphore_wait(ycred.at[s], 1)

        @pl.loop(0, GROUPS)
        def _(g):
            if turn == 0:
                load(g).wait()

            @pl.loop(0, per_group // 2)
            def _(p):
                c = g * per_group + 2 * p
                for t in range(2):
                    pair = [vext[c + i, pl.ds(k * CHUNK, window), pl.ds(t * TILE, TILE)].reshape(window * TILE, depth)
                            for i in range(2)]
                    got = jnp.dot(ax[t], jnp.concatenate(pair, axis=1), preferred_element_type=jnp.float32)
                    got = got.astype(jnp.bfloat16)
                    for i in range(2):
                        part = got[:, i * depth:(i + 1) * depth]
                        u1[c + i, pl.ds(k * CHUNK, CHUNK), pl.ds(t * TILE, TILE)] = part[:own].reshape(CHUNK, TILE, depth)
                        send[slot, t, c + i] = part[own:]

            for s in range(2):
                @pl.when(above[s][0])
                def _():
                    y_copy(k, slot, s, g).start()

        if n >= n_chunks - 2 and layer < n_layers - 1:
            @pl.when(beside[side][0])
            def _():
                pl.semaphore_signal(xcred.at[1 - side], inc=1, device_id=beside[side][1], device_id_type=MESH)

    def yz_pass(layer, n):
        k = chunk_of(n)
        chunk = pl.ds(k * CHUNK, CHUNK)

        @pl.loop(0, GROUPS)
        def _(g):
            for s in range(2):
                @pl.when(above[1 - s][0])
                def _():
                    y_copy(k, 0, s, g).wait_recv()

            @pl.loop(0, per_group // 8)
            def _(q):
                for h in range(4):
                    c = g * per_group + 8 * q + 2 * h
                    own = jnp.concatenate([u1[c + i, chunk].reshape(CHUNK * extent, depth) for i in range(2)], axis=1)
                    halo = jnp.concatenate([recv[k, c + i] for i in range(2)], axis=1)
                    rhs = jnp.concatenate([own, halo], axis=0)
                    u2 = jnp.dot(ay[...], rhs, preferred_element_type=jnp.float32).astype(jnp.bfloat16)
                    u3 = jnp.dot(u2, bz[...], preferred_element_type=jnp.float32).astype(jnp.bfloat16)
                    for i in range(2):
                        u1[c + i, chunk] = u3[:, i * depth:(i + 1) * depth].reshape(CHUNK, extent, depth)

        if layer < n_layers - 1:
            for s in range(2):
                @pl.when(above[s][0])
                def _():
                    pl.semaphore_signal(ycred.at[1 - s], inc=1, device_id=above[s][1], device_id_type=MESH)

    def mix(layer, n):
        k = chunk_of(n)

        @pl.loop(0, CHUNK // 2)
        def _(i):
            for s in range(2):
                x = k * CHUNK + 2 * i + s
                rhs = jnp.concatenate(
                    [u1[:, x, pl.ds(t * TILE, TILE)].reshape(chans * TILE, depth) for t in range(2)], axis=1)
                step = 256
                for m in range(chans * TILE // step):
                    acc = jnp.dot(wk[pl.ds(m * step, step)], rhs, preferred_element_type=jnp.float32)
                    cs = pl.ds(m * (step // TILE), step // TILE)
                    for t in range(2):
                        at = (cs, half + x, pl.ds(t * TILE, TILE))
                        pre = acc[:, t * depth:(t + 1) * depth] + bias[pl.ds(m * step, step)]
                        old = vext[at].reshape(step, depth).astype(jnp.float32)
                        vext[at] = (old + gelu(pre)).astype(jnp.bfloat16).reshape(step // TILE, TILE, depth)

        if layer == n_layers - 1:
            @pl.loop(0, chans)
            def _(c):
                u1[c, pl.ds(k * CHUNK, CHUNK)] = vext[c, pl.ds(half + k * CHUNK, CHUNK)]

    def send_halo(layer, n):
        side, which = side_of(n), {1: (3,), 2: (2,), 3: (0, 1)}[n // 2]
        if n // 2 == 1:
            @pl.when(beside[side][0])
            def _():
                pl.semaphore_wait(xcred.at[side], 1)
        x_start(side, which, layer + 1)

    for g in range(GROUPS):
        load(g).start()
    barrier = pltpu.get_barrier_semaphore()
    for dev in (left, right, up, down):
        pl.semaphore_signal(barrier, inc=1, device_id=dev, device_id_type=MESH)
    pl.semaphore_wait(barrier, 4)
    for piece in range(4):
        for side in range(2):
            x_start(side, (piece,), 0)
    set_x_matrices(0)
    x_pass(0, 0)

    for side in range(2):
        @pl.when(jnp.logical_not(beside[side][0]))
        def _():
            @pl.loop(0, chans)
            def _(c):
                vext[c, pl.ds(side * (half + planes), half)] = jnp.zeros((half, extent, depth), jnp.bfloat16)

        @pl.when(jnp.logical_not(above[side][0]))
        def _():
            @pl.loop(0, chans)
            def _(c):
                for k in range(n_chunks):
                    recv[k, c, pl.ds(side * slab, slab)] = jnp.zeros((slab, depth), jnp.bfloat16)

    last = n_chunks - 1
    early = 2
    for layer in range(n_layers):
        for n in range(1, n_chunks - 2):
            x_pass(layer, n)
        set_other_matrices(layer)

        @pl.loop(0, early)
        def _(n):
            yz_pass(layer, n)

        for n in range(n_chunks - 2, n_chunks):
            x_pass(layer, n)
        for side in range(2):
            @pl.when(beside[side][0])
            def _():
                for piece in range(4):
                    x_copy(side, piece, layer).wait_send()
        if layer < n_layers - 1:
            set_x_matrices(layer + 1)

        @pl.loop(0, last)
        def _(n):
            @pl.when(n >= early)
            def _():
                yz_pass(layer, n)

            mix(layer, n)
            if layer < n_layers - 1:
                for m in range(2, last):
                    @pl.when(n == m)
                    def _():
                        send_halo(layer, m)

        if layer < n_layers - 1:
            x_pass(layer + 1, 0)
        yz_pass(layer, last)
        mix(layer, last)
        if layer < n_layers - 1:
            send_halo(layer, last)

    turns = n_chunks * n_layers
    for turn in range(max(0, turns - SLOTS), turns):
        for s in range(2):
            @pl.when(above[s][0])
            def _():
                for g in range(GROUPS):
                    y_copy(chunk_of(turn % n_chunks), turn % SLOTS, s, g).wait_send()


def solution(mesh):
    nx, ny = mesh.shape[ROW_AXIS], mesh.shape[COL_AXIS]
    vol_spec = P(PARTS_AXIS, ROW_AXIS, COL_AXIS, None)

    def local_layers(volume, filter_taps, mix_weights, mix_bias):
        chans, planes, extent, depth = volume.shape
        half = (filter_taps.shape[2] - 1) // 2
        n_chunks, slab = planes // CHUNK, CHUNK * half
        bf = jnp.bfloat16
        return pl.pallas_call(
            functools.partial(stack_kernel, nx, ny),
            out_shape=pltpu.VMEM(volume.shape, bf),
            in_specs=[pl.BlockSpec(memory_space=pl.ANY), pl.BlockSpec(memory_space=pltpu.SMEM),
                      pl.BlockSpec(memory_space=pltpu.VMEM), pl.BlockSpec(memory_space=pltpu.VMEM)],
            out_specs=pl.BlockSpec(memory_space=pltpu.VMEM),
            scratch_shapes=[
                pltpu.VMEM((chans, planes + 2 * half, extent, depth), bf),
                pltpu.VMEM((SLOTS, 2, chans, slab, depth), bf),
                pltpu.VMEM((n_chunks, chans, 2 * slab, depth), bf),
                pltpu.VMEM((2, CHUNK * TILE + slab, (CHUNK + 2 * half) * TILE), bf),
                pltpu.VMEM((CHUNK * extent, CHUNK * extent + 2 * slab), bf),
                pltpu.VMEM((2 * depth, 2 * depth), bf),
                pltpu.VMEM((chans * TILE, chans * TILE), bf),
                pltpu.VMEM((chans * TILE, depth), jnp.float32),
                pltpu.SemaphoreType.DMA((GROUPS,)),
                pltpu.SemaphoreType.DMA((2, 4)),
                pltpu.SemaphoreType.DMA((2, 4)),
                pltpu.SemaphoreType.DMA((SLOTS, 2, GROUPS)),
                pltpu.SemaphoreType.DMA((n_chunks, 2, GROUPS)),
                pltpu.SemaphoreType.REGULAR((2,)),
                pltpu.SemaphoreType.REGULAR((2,)),
            ],
            compiler_params=pltpu.CompilerParams(
                collective_id=0, has_side_effects=True, vmem_limit_bytes=50200000),
            name="stack",
        )(volume, filter_taps, mix_weights, mix_bias)

    return jax.shard_map(local_layers, mesh=mesh, in_specs=(vol_spec, P(), P(), P()), out_specs=vol_spec, check_vma=False)
```

```python
import functools

import jax
import jax.numpy as jnp
from jax import lax
from jax.experimental import pallas as pl
from jax.experimental.pallas import tpu as pltpu
from jax.sharding import PartitionSpec as P

PARTS_AXIS = "batch"
COL_AXIS = "ysp"
ROW_AXIS = "xsp"
MESH = pl.DeviceIdType.MESH
TILE = 16
CHUNK = 4
GROUPS = 4
SLOTS = 5
X_UNROLL, Y_UNROLL = 8, 16


def rows_cols(n_rows, n_cols):
    shape = (n_rows, n_cols)
    return lax.broadcasted_iota(jnp.int32, shape, 0), lax.broadcasted_iota(jnp.int32, shape, 1)


def banded(tap, n_taps, tap_index, valid):
    index = jnp.where(valid, tap_index, -1)
    total = jnp.zeros(index.shape, jnp.float32)
    for t in range(n_taps):
        total = jnp.where(index == t, tap(t), total)
    return total.astype(jnp.bfloat16)


def x_matrix(tap, n_taps, last_tile):
    half = (n_taps - 1) // 2
    own = CHUNK * TILE
    r, k = rows_cols(own + CHUNK * half, (CHUNK + 2 * half) * TILE)
    s = jnp.maximum(r - own, 0)
    plane = jnp.where(r < own, r // TILE, s // half)
    row = jnp.where(r < own, r % TILE, s % half + (TILE - half if last_tile else 0))
    return banded(tap, n_taps, k // TILE - plane, row == k % TILE)


def y_matrix(tap, n_taps, extent):
    half = (n_taps - 1) // 2
    own, slab = CHUNK * extent, CHUNK * half
    r, k = rows_cols(own, own + 2 * slab)
    s = jnp.maximum(jnp.where(k < own + slab, k - own, k - own - slab), 0)
    plane = jnp.where(k < own, k // extent, s // half)
    pos = jnp.where(k < own, k % extent + half, jnp.where(k < own + slab, s % half, s % half + half + extent))
    return banded(tap, n_taps, pos - r % extent, plane == r // extent)


def z_matrix(tap, n_taps, depth):
    r, k = rows_cols(2 * depth, 2 * depth)
    return banded(tap, n_taps, r % depth - k % depth + (n_taps - 1) // 2, r // depth == k // depth)


def gelu(v):
    c0 = 0.7978845608028654
    arg = v * (c0 + (c0 * 0.044715) * (v * v))
    h = 0.5 * v
    return h + h * jnp.tanh(arg)


def stack_kernel(nx, ny, v_hbm, taps, weights, biases, u1, vext, send, recv, ax, ay, bz, wk, bias,
                 load_sem, xsend, xrecv, ysend, yrecv, ycred, xcred):
    chans, planes, extent, depth = u1.shape
    n_layers, _, n_taps = taps.shape
    half = (n_taps - 1) // 2
    n_chunks = planes // CHUNK
    middle = n_chunks // 2
    per_group = chans // GROUPS
    slab = CHUNK * half
    window = CHUNK + 2 * half
    near = half - 2 * CHUNK
    bi, yi, xi = lax.axis_index(PARTS_AXIS), lax.axis_index(COL_AXIS), lax.axis_index(ROW_AXIS)
    left = (bi, yi, lax.rem(xi + nx - 1, nx))
    right = (bi, yi, lax.rem(xi + 1, nx))
    up = (bi, lax.rem(yi + ny - 1, ny), xi)
    down = (bi, lax.rem(yi + 1, ny), xi)
    has_left, has_right, has_up, has_down = xi > 0, xi < nx - 1, yi > 0, yi < ny - 1
    beside = ((has_left, left), (has_right, right))
    above = ((has_up, up), (has_down, down))

    def side_of(n):
        return n % 2

    def chunk_of(n):
        return middle - 1 - n // 2 + side_of(n) * (1 + 2 * (n // 2))

    def load(g):
        cs = pl.ds(g * per_group, per_group)
        return pltpu.make_async_copy(v_hbm.at[cs], vext.at[cs, pl.ds(half, planes)], load_sem.at[g])

    pieces = ((0, near), (near, CHUNK - near), (CHUNK, CHUNK), (2 * CHUNK, near))

    def x_copy(side, piece, layer):
        first, n = pieces[piece]
        src = planes - first - n if side else first
        dst = src + half - planes if side else src + half + planes
        source = v_hbm.at[:, pl.ds(src, n)] if layer == 0 else vext.at[:, pl.ds(half + src, n)]
        return pltpu.make_async_remote_copy(
            src_ref=source, dst_ref=vext.at[:, pl.ds(dst, n)],
            send_sem=xsend.at[side, piece], recv_sem=xrecv.at[side, piece],
            device_id=beside[side][1], device_id_type=MESH)

    def x_start(side, which, layer):
        @pl.when(beside[side][0])
        def _():
            for piece in which:
                x_copy(side, piece, layer).start()

    def y_copy(k, slot, side, g):
        cs = pl.ds(g * per_group, per_group)
        return pltpu.make_async_remote_copy(
            src_ref=send.at[slot, side, cs], dst_ref=recv.at[k, cs, pl.ds((1 - side) * slab, slab)],
            send_sem=ysend.at[slot, side, g], recv_sem=yrecv.at[k, 1 - side, g],
            device_id=above[side][1], device_id_type=MESH)

    def set_x_matrices(layer):
        for t in range(2):
            ax[t] = x_matrix(lambda i: taps[layer, 0, i], n_taps, t == 1)

    def set_other_matrices(layer):
        ay[...] = y_matrix(lambda i: taps[layer, 1, i], n_taps, extent)
        bz[...] = z_matrix(lambda i: taps[layer, 2, i], n_taps, depth)
        block = 128

        @pl.loop(0, chans * TILE // block)
        def _(b):
            r, k = rows_cols(chans, chans * TILE)
            across = (k // TILE == r).astype(jnp.bfloat16)
            wide = jnp.dot(weights[layer].T, across, preferred_element_type=jnp.float32).astype(jnp.bfloat16)
            m, c = rows_cols(block, chans)
            mine = (m + b * block) // TILE == c
            full = jnp.dot(mine.astype(jnp.bfloat16), wide, preferred_element_type=jnp.float32)
            m, k = rows_cols(block, chans * TILE)
            at = pl.ds(pl.multiple_of(b * block, block), block)
            wk[at] = jnp.where(m % TILE == k % TILE, full, 0.0).astype(jnp.bfloat16)
            spread = jnp.sum(jnp.where(mine, biases[pl.ds(layer, 1)], 0.0), axis=1, keepdims=True)
            bias[at] = jnp.broadcast_to(spread, (block, depth))

    def x_pass(layer, n):
        k = chunk_of(n)
        own = CHUNK * TILE
        turn = n_chunks * layer + n
        slot = turn % SLOTS
        side = side_of(n)
        reach = {1: (0,), 2: (1, 2), 3: (3,)}.get(n // 2, ())
        if reach:
            @pl.when(beside[side][0])
            def _():
                for piece in reach:
                    x_copy(1 - side, piece, layer).wait_recv()
        for s in range(2):
            @pl.when(above[s][0])
            def _():
                if turn >= SLOTS:
                    for g in range(GROUPS):
                        y_copy(chunk_of((turn - SLOTS) % n_chunks), slot, s, g).wait_send()
                if layer > 0:
                    pl.semaphore_wait(ycred.at[s], 1)

        @pl.loop(0, GROUPS)
        def _(g):
            if turn == 0:
                load(g).wait()

            @pl.loop(0, per_group // X_UNROLL)
            def _(p):
                for h in range(X_UNROLL // 2):
                    c = g * per_group + X_UNROLL * p + 2 * h
                    for t in range(2):
                        pair = [vext[c + i, pl.ds(k * CHUNK, window), pl.ds(t * TILE, TILE)].reshape(window * TILE, depth)
                                for i in range(2)]
                        got = jnp.dot(ax[t], jnp.concatenate(pair, axis=1), preferred_element_type=jnp.float32)
                        got = got.astype(jnp.bfloat16)
                        for i in range(2):
                            part = got[:, i * depth:(i + 1) * depth]
                            u1[c + i, pl.ds(k * CHUNK, CHUNK), pl.ds(t * TILE, TILE)] = part[:own].reshape(
                                CHUNK, TILE, depth)
                            send[slot, t, c + i] = part[own:]

            for s in range(2):
                @pl.when(above[s][0])
                def _():
                    y_copy(k, slot, s, g).start()

        if n >= n_chunks - 2 and layer < n_layers - 1:
            @pl.when(beside[side][0])
            def _():
                pl.semaphore_signal(xcred.at[1 - side], inc=1, device_id=beside[side][1], device_id_type=MESH)

    def yz_pass(layer, n):
        k = chunk_of(n)
        chunk = pl.ds(k * CHUNK, CHUNK)

        @pl.loop(0, GROUPS)
        def _(g):
            for s in range(2):
                @pl.when(above[1 - s][0])
                def _():
                    y_copy(k, 0, s, g).wait_recv()

            @pl.loop(0, per_group // Y_UNROLL)
            def _(q):
                for h in range(Y_UNROLL // 2):
                    c = g * per_group + Y_UNROLL * q + 2 * h
                    own = jnp.concatenate([u1[c + i, chunk].reshape(CHUNK * extent, depth) for i in range(2)], axis=1)
                    halo = jnp.concatenate([recv[k, c + i] for i in range(2)], axis=1)
                    rhs = jnp.concatenate([own, halo], axis=0)
                    u2 = jnp.dot(ay[...], rhs, preferred_element_type=jnp.float32).astype(jnp.bfloat16)
                    u3 = jnp.dot(u2, bz[...], preferred_element_type=jnp.float32).astype(jnp.bfloat16)
                    for i in range(2):
                        u1[c + i, chunk] = u3[:, i * depth:(i + 1) * depth].reshape(CHUNK, extent, depth)

        if layer < n_layers - 1:
            for s in range(2):
                @pl.when(above[s][0])
                def _():
                    pl.semaphore_signal(ycred.at[1 - s], inc=1, device_id=above[s][1], device_id_type=MESH)

    def mix(layer, n):
        k = chunk_of(n)

        @pl.loop(0, CHUNK // 2)
        def _(i):
            for s in range(2):
                x = k * CHUNK + 2 * i + s
                rhs = jnp.concatenate(
                    [u1[:, x, pl.ds(t * TILE, TILE)].reshape(chans * TILE, depth) for t in range(2)], axis=1)
                step = 256
                for m in range(chans * TILE // step):
                    acc = jnp.dot(wk[pl.ds(m * step, step)], rhs, preferred_element_type=jnp.float32)
                    cs = pl.ds(m * (step // TILE), step // TILE)
                    for t in range(2):
                        at = (cs, half + x, pl.ds(t * TILE, TILE))
                        pre = acc[:, t * depth:(t + 1) * depth] + bias[pl.ds(m * step, step)]
                        old = vext[at].reshape(step, depth).astype(jnp.float32)
                        vext[at] = (old + gelu(pre)).astype(jnp.bfloat16).reshape(step // TILE, TILE, depth)

        if layer == n_layers - 1:
            @pl.loop(0, chans)
            def _(c):
                u1[c, pl.ds(k * CHUNK, CHUNK)] = vext[c, pl.ds(half + k * CHUNK, CHUNK)]

    def send_halo(layer, n):
        side, which = side_of(n), {1: (3,), 2: (2,), 3: (0, 1)}[n // 2]
        if n // 2 == 1:
            @pl.when(beside[side][0])
            def _():
                pl.semaphore_wait(xcred.at[side], 1)
        x_start(side, which, layer + 1)

    for g in range(GROUPS):
        load(g).start()
    barrier = pltpu.get_barrier_semaphore()
    for dev in (left, right, up, down):
        pl.semaphore_signal(barrier, inc=1, device_id=dev, device_id_type=MESH)
    pl.semaphore_wait(barrier, 4)
    for piece in range(4):
        for side in range(2):
            x_start(side, (piece,), 0)
    set_x_matrices(0)
    x_pass(0, 0)

    for side in range(2):
        @pl.when(jnp.logical_not(beside[side][0]))
        def _():
            @pl.loop(0, chans)
            def _(c):
                vext[c, pl.ds(side * (half + planes), half)] = jnp.zeros((half, extent, depth), jnp.bfloat16)

        @pl.when(jnp.logical_not(above[side][0]))
        def _():
            @pl.loop(0, chans)
            def _(c):
                for k in range(n_chunks):
                    recv[k, c, pl.ds(side * slab, slab)] = jnp.zeros((slab, depth), jnp.bfloat16)

    last = n_chunks - 1
    early = {n_chunks - 4: 0, n_chunks - 2: 1}
    for layer in range(n_layers):
        for n in range(1, n_chunks):
            if n == 2:
                set_other_matrices(layer)
            if n in early:
                yz_pass(layer, early[n])
            x_pass(layer, n)
        for side in range(2):
            @pl.when(beside[side][0])
            def _():
                for piece in range(4):
                    x_copy(side, piece, layer).wait_send()
        if layer < n_layers - 1:
            set_x_matrices(layer + 1)

        @pl.loop(0, last)
        def _(n):
            @pl.when(n >= len(early))
            def _():
                yz_pass(layer, n)

            mix(layer, n)
            if layer < n_layers - 1:
                for m in range(2, last):
                    @pl.when(n == m)
                    def _():
                        send_halo(layer, m)

        if layer < n_layers - 1:
            x_pass(layer + 1, 0)
        yz_pass(layer, last)
        mix(layer, last)
        if layer < n_layers - 1:
            send_halo(layer, last)

    turns = n_chunks * n_layers
    for turn in range(max(0, turns - SLOTS), turns):
        for s in range(2):
            @pl.when(above[s][0])
            def _():
                for g in range(GROUPS):
                    y_copy(chunk_of(turn % n_chunks), turn % SLOTS, s, g).wait_send()


def solution(mesh):
    nx, ny = mesh.shape[ROW_AXIS], mesh.shape[COL_AXIS]
    vol_spec = P(PARTS_AXIS, ROW_AXIS, COL_AXIS, None)

    def local_layers(volume, filter_taps, mix_weights, mix_bias):
        chans, planes, extent, depth = volume.shape
        half = (filter_taps.shape[2] - 1) // 2
        n_chunks, slab = planes // CHUNK, CHUNK * half
        bf = jnp.bfloat16
        return pl.pallas_call(
            functools.partial(stack_kernel, nx, ny),
            out_shape=pltpu.VMEM(volume.shape, bf),
            in_specs=[pl.BlockSpec(memory_space=pl.ANY), pl.BlockSpec(memory_space=pltpu.SMEM),
                      pl.BlockSpec(memory_space=pltpu.VMEM), pl.BlockSpec(memory_space=pltpu.VMEM)],
            out_specs=pl.BlockSpec(memory_space=pltpu.VMEM),
            scratch_shapes=[
                pltpu.VMEM((chans, planes + 2 * half, extent, depth), bf),
                pltpu.VMEM((SLOTS, 2, chans, slab, depth), bf),
                pltpu.VMEM((n_chunks, chans, 2 * slab, depth), bf),
                pltpu.VMEM((2, CHUNK * TILE + slab, (CHUNK + 2 * half) * TILE), bf),
                pltpu.VMEM((CHUNK * extent, CHUNK * extent + 2 * slab), bf),
                pltpu.VMEM((2 * depth, 2 * depth), bf),
                pltpu.VMEM((chans * TILE, chans * TILE), bf),
                pltpu.VMEM((chans * TILE, depth), jnp.float32),
                pltpu.SemaphoreType.DMA((GROUPS,)),
                pltpu.SemaphoreType.DMA((2, 4)),
                pltpu.SemaphoreType.DMA((2, 4)),
                pltpu.SemaphoreType.DMA((SLOTS, 2, GROUPS)),
                pltpu.SemaphoreType.DMA((n_chunks, 2, GROUPS)),
                pltpu.SemaphoreType.REGULAR((2,)),
                pltpu.SemaphoreType.REGULAR((2,)),
            ],
            compiler_params=pltpu.CompilerParams(
                collective_id=0, has_side_effects=True, vmem_limit_bytes=50200000),
            name="stack",
        )(volume, filter_taps, mix_weights, mix_bias)

    return jax.shard_map(local_layers, mesh=mesh, in_specs=(vol_spec, P(), P(), P()), out_specs=vol_spec, check_vma=False)
```
